32 devices in a mesh: grp: 4 (over y, x), dev: 8 (over z, core).
Axes of the slice: x: 2, y: 2, z: 4, core: 2. Of those that a mesh axis runs over, the one named last changes fastest.
Arguments:
- table: float32 [262144, 128], P(('grp', 'dev')), may hold values from -6 to 6
- cold_grads: float32 [131072, 128], P(('grp', 'dev')), may hold values from -6 to 6
- cold_owner: int32 [131072, 1], P(('grp', 'dev')), may hold values from 0 to 31; in each aligned block of 4096 rows (0 to 4095, 4096 to 8191, ...) at most 256 rows name the same one
- cold_row: int32 [131072], P(('grp', 'dev')), may hold values from 0 to 8191
- hot_grads: float32 [32768, 128], P(('grp', 'dev')), may hold values from -6 to 6
- hot_slot: int32 [32768], P(('grp', 'dev')), may hold values from 0 to 255
- hot_ids: int32 [256], replicated, may hold values from 0 to 262143, as said below
Outputs:
- new_table: float32 [262144, 128], P(('grp', 'dev'))
The draws below stay inside these ranges and needn't reach their ends.
Inputs may be any that keep to these rules, and one draw needn't show every extreme that they name: `cold_owner`: among the 4096 rare-row lookups of one device no owner is named more than 256 times, a bound that some block reaches. `hot_ids`: all entries differ.
All inputs are finite; a program needn't handle non-finite values.
Results may differ from the reference program's by a relative error of at most 0.00005.
Values sent between devices are 32-bit elements; how exact they have to be, the bound alone decides.
A program may use at most 64 MiB of HBM per device.

```python
import math
import jax
import jax.numpy as jnp
import numpy as np

W = 128
ROWS_DEV = 8192
HOT = 256
COLD_DEV = 4096
CAP = 256
ROWS = 262144
COLD = 131072
HOT_LOOK = 32768
DEVICES = 32


def draw_hot_ids(key, part):
    return jax.random.choice(jax.random.fold_in(key, 7), ROWS, (HOT,), replace=False).astype(jnp.int32)


def plant(array, own_key, smallest, largest):
    index_at = [jax.random.randint(jax.random.fold_in(own_key, axis), (), 0, length) for axis, length in enumerate(array.shape)]
    longest = array.shape.index(max(array.shape))
    next_to = index_at[:longest] + [(index_at[longest] + 1) % array.shape[longest]] + index_at[longest + 1:]
    return array.at[tuple(index_at)].set(smallest).at[tuple(next_to)].set(largest)


def block_scale(own_key, shape, shards, low, high):
    level = 1.0
    for axis_at, blocks in shards:
        heights = jax.random.uniform(jax.random.fold_in(jax.random.fold_in(own_key, 6), axis_at), (blocks,), jnp.float32, low / len(shards), high / len(shards))
        level = level * jnp.repeat(jnp.exp(heights), shape[axis_at] // blocks).reshape((-1,) + (1,) * (len(shape) - 1 - axis_at))
    return level


def deal_out(stream_key, own, number, rows, count, top, most, lean):
    order = jax.random.permutation(stream_key, count)
    packed, common = shares(count, rows * top, most, lean, True), shares(count, rows * top, most, lean, False)
    places = jnp.arange(count)

    def named(sizes, rotation):
        used = int((sizes > 0).sum())
        fixed = max(1, used // 4)
        moved = fixed + (places - fixed + rotation * (used - fixed)) % max(1, count - fixed)
        return jnp.zeros((count,), jnp.int32).at[order[jnp.where(places < fixed, places, moved)]].set(jnp.asarray(sizes, jnp.int32))

    sizes = jnp.where(number % 4 == 0, named(packed, number // 4), named(common, number - number // 4 - 1))
    mixed = jax.random.permutation(jax.random.fold_in(own, 3), count)
    donor, sink = mixed[0:count // 2 * 2:2], mixed[1:count // 2 * 2:2]
    room = jnp.minimum(sizes[donor] - 1, most - sizes[sink]) // 2
    room = jnp.where((donor == order[0]) | (sink == order[0]) | (sizes[sink] == 0), 0, jnp.maximum(room, 0))
    moved = jax.random.randint(jax.random.fold_in(own, 4), (count // 2,), 0, 1 << 20) % (room + 1)
    sizes = sizes.at[donor].add(-moved).at[sink].add(moved)
    members = jnp.searchsorted(jnp.cumsum(sizes), jnp.arange(rows * top), side="right").astype(jnp.int32)
    grid = members.reshape(top, rows).T
    grid = grid[jax.random.permutation(jax.random.fold_in(own, 1), rows)]
    rotation = jax.random.randint(jax.random.fold_in(own, 2), (rows, 1), 0, top)
    return jnp.take_along_axis(grid, (jnp.arange(top)[None, :] + rotation) % top, axis=1)


def shares(count, total, reach, lean, full):
    loads = [(1 << 20) // math.isqrt(grade ** lean) + 1 for grade in range(1, count + 1)]
    largest = reach if full else min(reach, max(-(-total // count), total * loads[0] // sum(loads)))
    least = 1 if total - largest >= count - 1 else 0
    holding, surplus = [largest] + [least] * (count - 1), total - largest - least * (count - 1)
    while surplus > 0:
        free = [i for i in range(1, count) if holding[i] < largest] or [i for i in range(1, count) if holding[i] < reach]
        pool, left = sum([loads[i] for i in free]), surplus
        for i in free:
            addition = min(reach - holding[i], max(1, left * loads[i] // pool), surplus)
            holding[i] = holding[i] + addition
            surplus = surplus - addition
    return np.array(holding)


def gaussian(stream_key, extent, scale, bound, split=(), kind=jnp.bfloat16):
    values = scale * jax.random.normal(stream_key, extent, jnp.float32)
    if split:
        values = values * block_scale(stream_key, extent, split, -0.22, 0.18)
    return jnp.clip(values, -bound, bound).astype(kind)


def setup_inputs(seed: int = 0) -> dict:
    key_list = jax.random.split(jax.random.key(seed), 8)
    table = gaussian(key_list[0], (ROWS, W), 1.0, 6.0, ((0, 32),), jnp.float32)
    cold_grads = gaussian(key_list[1], (COLD, W), 1.0, 6.0, ((0, 32),), jnp.float32)
    cold_owner_keys = jax.random.split(jax.random.fold_in(key_list[2], 1), COLD // COLD_DEV)
    cold_owner_turns = jax.random.permutation(jax.random.fold_in(key_list[2], 3), COLD // COLD_DEV)
    cold_owner = jax.vmap(lambda own, number: deal_out(jax.random.fold_in(key_list[2], 2), own, number, COLD_DEV, DEVICES, 1, CAP, 2))(cold_owner_keys, cold_owner_turns).reshape((COLD, 1))
    cold_row = plant(jax.random.randint(key_list[3], (COLD,), 0, ROWS_DEV), jax.random.fold_in(key_list[3], 1), 0, ROWS_DEV - 1).astype(jnp.int32)
    hot_grads = gaussian(key_list[4], (HOT_LOOK, W), 1.0, 6.0, ((0, 32),), jnp.float32)
    hot_slot = plant(jax.random.randint(key_list[5], (HOT_LOOK,), 0, HOT), jax.random.fold_in(key_list[5], 1), 0, HOT - 1).astype(jnp.int32)
    hot_ids = draw_hot_ids(jax.random.fold_in(key_list[7], 71), 0)
    return {"table": table, "cold_grads": cold_grads, "cold_owner": cold_owner, "cold_row": cold_row, "hot_grads": hot_grads, "hot_slot": hot_slot, "hot_ids": hot_ids}


def reference(table, cold_grads, cold_owner, cold_row, hot_grads, hot_slot, hot_ids):
    cold_id = (cold_owner[:, 0] * ROWS_DEV + cold_row).astype(jnp.int32)
    hot_id = hot_ids[hot_slot].astype(jnp.int32)
    new_table = table.at[cold_id].add(-0.05 * cold_grads)
    new_table = new_table.at[hot_id].add(-0.05 * hot_grads)
    return new_table
```

```python
import functools

import jax
import jax.numpy as jnp
from jax import lax
from jax.experimental import pallas as pl
from jax.experimental.pallas import tpu as pltpu
from jax.sharding import PartitionSpec as P

LEARN = 0.05
MESH = pl.DeviceIdType.MESH
LANES = 128
CHUNK = 256
WAYS = 4
TILE = 1024


def plan_kernel(slots, owner_ref, hot_grads_ref, hot_slot_ref, place_ref, count_ref, partial_ref):
    lookups = owner_ref.shape[0]
    wide = count_ref.shape[1]
    above = lax.broadcasted_iota(jnp.int32, (CHUNK, CHUNK), 0)
    below = lax.broadcasted_iota(jnp.int32, (CHUNK, CHUNK), 1)
    tri = (above >= below).astype(jnp.bfloat16)
    owners = lax.broadcasted_iota(jnp.int32, (CHUNK, wide), 1)
    start = owners.astype(jnp.float32) * slots - 1.0
    ones = jnp.ones((8, wide), jnp.float32)
    base = jnp.zeros((1, wide), jnp.float32)
    for b in range(lookups // CHUNK):
        hit = owner_ref[b * CHUNK:(b + 1) * CHUNK, :] == owners
        run = jnp.dot(tri, hit.astype(jnp.bfloat16), preferred_element_type=jnp.float32) + base
        base = run[CHUNK - 1:CHUNK, :]
        chosen = jnp.where(hit, run + start, 0.0)
        flat = lax.dot_general(
            ones, chosen, (((1,), (1,)), ((), ())),
            precision=lax.Precision.HIGHEST, preferred_element_type=jnp.float32,
        )
        whole = (flat + 0.5).astype(jnp.int32)
        for j in range(CHUNK // LANES):
            r = b * (CHUNK // LANES) + j
            place_ref[r:r + 1, :] = whole[0:1, j * LANES:(j + 1) * LANES]
    count_ref[...] = jnp.broadcast_to((base + 0.5).astype(jnp.int32), count_ref.shape)
    hot = partial_ref.shape[0]
    looks = hot_grads_ref.shape[0]
    pick = lax.broadcasted_iota(jnp.int32, (hot, looks), 0) == hot_slot_ref[...]
    partial_ref[...] = jnp.dot(
        pick.astype(jnp.float32), hot_grads_ref[...],
        precision=lax.Precision.HIGHEST, preferred_element_type=jnp.float32,
    )


def pack_kernel(place_ref, row_ref, grads_ref, send_ref, rows_ref):
    step = 16

    def body(t, carry):
        first = pl.multiple_of(t * step, step)
        for j in range(step):
            to = place_ref[first + j]
            rows_ref[to] = row_ref[first + j]
            send_ref[pl.ds(to, 1), :] = grads_ref[pl.ds(first + j, 1), :]
        return carry

    lax.fori_loop(0, grads_ref.shape[0] // step, body, 0)


def exchange_kernel(
    n_grp, n_dev, send_ref, meta_ref, part_ref, got_ref, gmeta_ref, total_ref,
    rbuf, s_big, r_big, s_meta, r_meta, s_rs, r_rs, s_ag, r_ag, s_own,
):
    devices = n_grp * n_dev
    me = lax.axis_index("grp") * n_dev + lax.axis_index("dev")
    barrier = pltpu.get_barrier_semaphore()

    def peer(k):
        p = lax.rem(me + k, devices)
        return p, (p // n_dev, lax.rem(p, n_dev))

    def each(fn):
        def body(k, carry):
            fn(*peer(k))
            return carry
        lax.fori_loop(1, devices, body, 0)

    def remote(src, dst, ssem, rsem, where):
        return pltpu.make_async_remote_copy(
            src_ref=src, dst_ref=dst, send_sem=ssem, recv_sem=rsem,
            device_id=where, device_id_type=MESH,
        )

    each(lambda p, w: pl.semaphore_signal(barrier, inc=1, device_id=w, device_id_type=MESH))
    pl.semaphore_wait(barrier, devices - 1)

    each(lambda p, w: remote(part_ref.at[p], rbuf.at[me], s_rs, r_rs, w).start())
    each(lambda p, w: remote(meta_ref.at[p], gmeta_ref.at[me], s_meta, r_meta, w).start())
    each(lambda p, w: remote(send_ref.at[p], got_ref.at[me], s_big, r_big, w).start())
    own_big = pltpu.make_async_copy(send_ref.at[me], got_ref.at[me], s_own.at[0])
    own_meta = pltpu.make_async_copy(meta_ref.at[me], gmeta_ref.at[me], s_own.at[1])
    own_big.start()
    own_meta.start()
    rbuf[me] = part_ref[me]

    here = (lax.axis_index("grp"), lax.axis_index("dev"))
    most = pl.ds(0, devices - 1)

    def all_of(src, dst, ssem, rsem):
        return remote(src.at[most], dst.at[most], ssem, rsem, here)

    rs = all_of(part_ref, rbuf, s_rs, r_rs)
    rs.wait_recv()
    total_ref[me] = jnp.sum(rbuf[...], axis=0)
    rs.wait_send()
    each(lambda p, w: remote(total_ref.at[me], total_ref.at[me], s_ag, r_ag, w).start())
    for t in (
        all_of(meta_ref, gmeta_ref, s_meta, r_meta),
        all_of(send_ref, got_ref, s_big, r_big),
        all_of(total_ref, total_ref, s_ag, r_ag),
    ):
        t.wait_send()
        t.wait_recv()
    own_big.wait()
    own_meta.wait()


def apply_kernel(
    slots, rows_ref, count_ref, local_ref, table_ref, got_ref, hot_ref, out_ref,
    grads, base, acc, g_sem, t_sem, o_sem,
):
    devices = got_ref.shape[0]
    rows_dev = table_ref.shape[0]
    for s in range(devices):
        pltpu.make_async_copy(got_ref.at[s], grads.at[s], g_sem.at[s]).start()
    load = pltpu.make_async_copy(table_ref, base, t_sem)
    load.start()

    def clear(t, carry):
        r = pl.ds(pl.multiple_of(t * 64, 64), 64)
        for a in acc:
            a[r, :] = jnp.zeros((64, a.shape[1]), jnp.float32)
        return carry

    lax.fori_loop(0, rows_dev // 64, clear, 0)

    def add(pairs):
        olds = [acc[j % WAYS][pl.ds(i, 1), :] for j, (i, _) in enumerate(pairs)]
        news = [o + g() for o, (_, g) in zip(olds, pairs)]
        for j, ((i, _), v) in enumerate(zip(pairs, news)):
            acc[j % WAYS][pl.ds(i, 1), :] = v

    def source(s, carry):
        pltpu.make_async_copy(got_ref.at[s], grads.at[s], g_sem.at[s]).wait()
        n = count_ref[s]
        first = s * slots

        def entry(i):
            return rows_ref[first + i], lambda: grads[s, pl.ds(i, 1), :]

        def four(t, c):
            for u in range(2):
                add([entry(t * 2 * WAYS + u * WAYS + j) for j in range(WAYS)])
            return c

        def one(i, c):
            add([entry(i)])
            return c

        full = n // (2 * WAYS)
        lax.fori_loop(0, full, four, 0)
        lax.fori_loop(full * 2 * WAYS, n, one, 0)
        return carry

    lax.fori_loop(0, devices, source, 0)

    def hot_one(i, c):
        r = local_ref[i]

        @pl.when((r >= 0) & (r < rows_dev))
        def _():
            add([(r, lambda: hot_ref[pl.ds(i, 1), :])])

        return c

    lax.fori_loop(0, local_ref.shape[0], hot_one, 0)
    load.wait()
    parts = 4
    size = rows_dev // parts
    outs = []
    for q in range(parts):
        def finish(t, c):
            r = pl.ds(pl.multiple_of(q * size + t * 64, 64), 64)
            v = acc[0][r, :]
            for a in acc[1:]:
                v = v + a[r, :]
            base[r, :] = base[r, :] - LEARN * v
            return c

        lax.fori_loop(0, size // 64, finish, 0)
        w = pl.ds(q * size, size)
        outs.append(pltpu.make_async_copy(base.at[w], out_ref.at[w], o_sem.at[q]))
        outs[-1].start()
    for o in outs:
        o.wait()


def on_device(n_grp, n_dev, table, cold_grads, cold_owner, cold_row, hot_grads, hot_slot, hot_ids):
    devices = n_grp * n_dev
    width = table.shape[1]
    lookups = cold_grads.shape[0]
    rows_dev = table.shape[0]
    hot = hot_ids.shape[0]
    slots = max(4, 2 * lookups // devices)
    wide = -(-devices // LANES) * LANES
    vmem, smem, hbm = (pl.BlockSpec(memory_space=m) for m in (pltpu.VMEM, pltpu.SMEM, pl.ANY))
    f32, i32 = jnp.float32, jnp.int32
    place, count, partial = pl.pallas_call(
        functools.partial(plan_kernel, slots),
        out_shape=(
            jax.ShapeDtypeStruct((lookups // LANES, LANES), i32),
            jax.ShapeDtypeStruct((8, wide), i32),
            jax.ShapeDtypeStruct((hot, width), f32),
        ),
        in_specs=[vmem] * 3,
        out_specs=(vmem,) * 3,
        name="plan",
    )(cold_owner, hot_grads, hot_slot.reshape(1, -1))
    send, rows = pl.pallas_call(
        pack_kernel,
        out_shape=(
            jax.ShapeDtypeStruct((devices * slots, width), f32),
            jax.ShapeDtypeStruct((devices * slots,), i32),
        ),
        in_specs=[smem, smem, vmem],
        out_specs=(vmem, smem),
        name="pack",
    )(place.reshape(-1), cold_row, cold_grads)
    span = -(-(slots + 1) // TILE) * TILE
    meta = jnp.concatenate(
        [rows.reshape(devices, slots), count[0, :devices, None],
         jnp.zeros((devices, span - slots - 1), i32)], axis=1,
    ).reshape(devices, span // LANES, LANES)
    share = -(-hot // devices)
    partial = jnp.pad(partial, ((0, share * devices - hot), (0, 0))).reshape(devices, share, width)
    dma = pltpu.SemaphoreType.DMA
    got, gmeta, total = pl.pallas_call(
        functools.partial(exchange_kernel, n_grp, n_dev),
        out_shape=(
            jax.ShapeDtypeStruct((devices, slots, width), f32),
            jax.ShapeDtypeStruct(meta.shape, i32),
            jax.ShapeDtypeStruct(partial.shape, f32),
        ),
        in_specs=[hbm, hbm, vmem],
        out_specs=(hbm, hbm, vmem),
        scratch_shapes=[pltpu.VMEM(partial.shape, f32)] + [dma] * 8 + [dma((2,))],
        compiler_params=pltpu.CompilerParams(collective_id=0, has_side_effects=True),
        name="exchange",
    )(send.reshape(devices, slots, width), meta, partial)
    gflat = gmeta.reshape(devices, span)
    me = lax.axis_index("grp") * n_dev + lax.axis_index("dev")
    return pl.pallas_call(
        functools.partial(apply_kernel, slots),
        out_shape=jax.ShapeDtypeStruct(table.shape, f32),
        in_specs=[smem, smem, smem, hbm, hbm, vmem],
        out_specs=hbm,
        scratch_shapes=[
            pltpu.VMEM(got.shape, f32),
            pltpu.VMEM(table.shape, f32),
            [pltpu.VMEM(table.shape, f32) for _ in range(WAYS)],
            dma((devices,)), dma, dma((4,)),
        ],
        compiler_params=pltpu.CompilerParams(vmem_limit_bytes=48 * 1024 * 1024),
        name="apply",
    )(gflat[:, :slots].reshape(-1), gflat[:, slots], hot_ids - me * rows_dev,
      table, got, total.reshape(-1, width))


def solution(mesh):
    in_specs = (
        P(("grp", "dev"), None),
        P(("grp", "dev"), None),
        P(("grp", "dev"), None),
        P(("grp", "dev")),
        P(("grp", "dev"), None),
        P(("grp", "dev")),
        P(),
    )
    out_specs = P(("grp", "dev"), None)
    return jax.shard_map(
        functools.partial(on_device, mesh.shape["grp"], mesh.shape["dev"]),
        mesh=mesh, in_specs=in_specs, out_specs=out_specs, check_vma=False,
    )
```

```python
import functools

import jax
import jax.numpy as jnp
from jax import lax
from jax.experimental import pallas as pl
from jax.experimental.pallas import tpu as pltpu
from jax.sharding import PartitionSpec as P

LEARN = 0.05
MESH = pl.DeviceIdType.MESH
LANES = 128
CHUNK = 256


def plan_kernel(slots, owner_ref, hot_grads_ref, hot_slot_ref, place_ref, count_ref, partial_ref):
    lookups = owner_ref.shape[0]
    wide = count_ref.shape[1]
    above = lax.broadcasted_iota(jnp.int32, (CHUNK, CHUNK), 0)
    below = lax.broadcasted_iota(jnp.int32, (CHUNK, CHUNK), 1)
    tri = (above >= below).astype(jnp.bfloat16)
    owners = lax.broadcasted_iota(jnp.int32, (CHUNK, wide), 1)
    start = owners.astype(jnp.float32) * slots - 1.0
    ones = jnp.ones((8, wide), jnp.float32)
    base = jnp.zeros((1, wide), jnp.float32)
    for b in range(lookups // CHUNK):
        hit = owner_ref[b * CHUNK:(b + 1) * CHUNK, :] == owners
        run = jnp.dot(tri, hit.astype(jnp.bfloat16), preferred_element_type=jnp.float32) + base
        base = run[CHUNK - 1:CHUNK, :]
        chosen = jnp.where(hit, run + start, 0.0)
        flat = lax.dot_general(
            ones, chosen, (((1,), (1,)), ((), ())),
            precision=lax.Precision.HIGHEST, preferred_element_type=jnp.float32,
        )
        whole = (flat + 0.5).astype(jnp.int32)
        for j in range(CHUNK // LANES):
            r = b * (CHUNK // LANES) + j
            place_ref[r:r + 1, :] = whole[0:1, j * LANES:(j + 1) * LANES]
    count_ref[...] = jnp.broadcast_to((base + 0.5).astype(jnp.int32), count_ref.shape)
    hot = partial_ref.shape[0]
    looks = hot_grads_ref.shape[0]
    pick = lax.broadcasted_iota(jnp.int32, (hot, looks), 0) == hot_slot_ref[...]
    partial_ref[...] = jnp.dot(
        pick.astype(jnp.float32), hot_grads_ref[...],
        precision=lax.Precision.HIGHEST, preferred_element_type=jnp.float32,
    )


def pack_kernel(place_ref, row_ref, grads_ref, send_ref, rows_ref):
    step = 16

    def body(t, carry):
        first = pl.multiple_of(t * step, step)
        for j in range(step):
            to = place_ref[first + j]
            rows_ref[to] = row_ref[first + j]
            send_ref[pl.ds(to, 1), :] = grads_ref[pl.ds(first + j, 1), :]
        return carry

    lax.fori_loop(0, grads_ref.shape[0] // step, body, 0)


def exchange_kernel(
    n_grp, n_dev, slots, send_ref, meta_ref, part_ref, local_ref, table_ref, out_ref,
    got, gmeta, total, rbuf, acc, halves, s_big, r_big, s_meta, r_meta, s_rs, r_rs, s_ag, r_ag, s_own,
):
    devices = n_grp * n_dev
    width = acc.shape[1]
    rows_dev = acc.shape[0]
    tile = min(1024, rows_dev)
    me = lax.axis_index("grp") * n_dev + lax.axis_index("dev")
    barrier = pltpu.get_barrier_semaphore()

    def each(fn, first=1, last=devices):
        def body(k, carry):
            p = lax.rem(me + k, devices)
            fn(k, p, (p // n_dev, lax.rem(p, n_dev)))
            return carry
        lax.fori_loop(first, last, body, 0)

    def remote(src, dst, ssem, rsem, where):
        return pltpu.make_async_remote_copy(
            src_ref=src, dst_ref=dst, send_sem=ssem, recv_sem=rsem,
            device_id=where, device_id_type=MESH,
        )

    load = pltpu.make_async_copy(table_ref, acc, s_own.at[0])
    load.start()
    own_big = pltpu.make_async_copy(send_ref.at[me], got.at[me], s_own.at[1])
    own_big.start()
    each(lambda k, p, w: pl.semaphore_signal(barrier, inc=1, device_id=w, device_id_type=MESH))
    pl.semaphore_wait(barrier, devices - 1)

    def big(k, p, w):
        remote(send_ref.at[p], got.at[me], s_big, r_big.at[k], w).start()

    half = devices // 2
    each(lambda k, p, w: remote(part_ref.at[p], rbuf.at[me], s_rs, r_rs, w).start())
    each(lambda k, p, w: remote(meta_ref.at[p], gmeta.at[me], s_meta, r_meta, w).start())
    each(big, 1, half)
    rbuf[me] = part_ref[me]
    gmeta[me] = meta_ref[me]

    here = (lax.axis_index("grp"), lax.axis_index("dev"))
    most = pl.ds(0, devices - 1)

    def all_of(src, dst, ssem, rsem):
        return remote(src.at[most], dst.at[most], ssem, rsem, here)

    rs = all_of(part_ref, rbuf, s_rs, r_rs)
    rs.wait_recv()
    total[me] = jnp.sum(rbuf[...], axis=0)
    each(big, half, half + half // 2)
    rs.wait_send()
    each(lambda k, p, w: remote(total.at[me], total.at[me], s_ag, r_ag, w).start())
    each(big, half + half // 2, devices)

    def add(values, ids):
        count = values.shape[0]
        high = values.astype(jnp.bfloat16)
        halves[0:count, 0:width] = high
        halves[0:count, width:2 * width] = (values - high.astype(jnp.float32)).astype(jnp.bfloat16)
        spot = lax.broadcasted_iota(jnp.int32, (tile, count), 0)

        def body(t, carry):
            at = pl.multiple_of(t * tile, tile)
            hit = jnp.where(spot == ids - at, 1.0, 0.0).astype(jnp.bfloat16)
            both = jnp.dot(hit, halves[0:count, :], preferred_element_type=jnp.float32)
            w = pl.ds(at, tile)
            acc[w, :] = acc[w, :] - LEARN * (both[:, :width] + both[:, width:])
            return carry

        lax.fori_loop(0, rows_dev // tile, body, 0)

    lines = -(-slots // LANES)

    def add_block(source):
        info = gmeta[source]
        filled = info[lines:lines + 1, :]
        ids = jnp.concatenate([info[j:j + 1, :] for j in range(lines)], axis=1)[:, :slots]
        held = jnp.concatenate([filled] * lines, axis=1)[:, :slots]
        ids = jnp.where(lax.broadcasted_iota(jnp.int32, (1, slots), 1) < held, ids, -1)
        block = got[source]
        deep = lax.broadcasted_iota(jnp.int32, block.shape, 0)
        add(jnp.where(deep < filled[:, :width], block, 0.0), ids)

    load.wait()
    own_big.wait()
    add_block(me)
    metas = all_of(meta_ref, gmeta, s_meta, r_meta)
    metas.wait_send()
    metas.wait_recv()

    def arrived(k, carry):
        source = lax.rem(me - k + devices, devices)
        remote(send_ref.at[0], got.at[source], s_big, r_big.at[k], here).wait_recv()
        add_block(source)
        return carry

    lax.fori_loop(1, devices, arrived, 0)
    ag = all_of(total, total, s_ag, r_ag)
    ag.wait_send()
    ag.wait_recv()
    hot = local_ref.shape[1]
    add(total[...].reshape(-1, width)[:hot], local_ref[...])
    out = pltpu.make_async_copy(acc, out_ref, s_own.at[0])
    out.start()
    remote(send_ref.at[most], got.at[most], s_big, r_big.at[0], here).wait_send()
    out.wait()


def on_device(n_grp, n_dev, table, cold_grads, cold_owner, cold_row, hot_grads, hot_slot, hot_ids):
    devices = n_grp * n_dev
    width = table.shape[1]
    lookups = cold_grads.shape[0]
    rows_dev = table.shape[0]
    hot = hot_ids.shape[0]
    slots = max(4, 2 * lookups // devices)
    wide = -(-devices // LANES) * LANES
    vmem, smem, hbm = (pl.BlockSpec(memory_space=m) for m in (pltpu.VMEM, pltpu.SMEM, pl.ANY))
    f32, i32 = jnp.float32, jnp.int32
    place, count, partial = pl.pallas_call(
        functools.partial(plan_kernel, slots),
        out_shape=(
            jax.ShapeDtypeStruct((lookups // LANES, LANES), i32),
            jax.ShapeDtypeStruct((8, wide), i32),
            jax.ShapeDtypeStruct((hot, width), f32),
        ),
        in_specs=[vmem] * 3,
        out_specs=(vmem,) * 3,
        name="plan",
    )(cold_owner, hot_grads, hot_slot.reshape(1, -1))
    send, rows = pl.pallas_call(
        pack_kernel,
        out_shape=(
            jax.ShapeDtypeStruct((devices * slots, width), f32),
            jax.ShapeDtypeStruct((devices * slots,), i32),
        ),
        in_specs=[smem, smem, vmem],
        out_specs=(vmem, smem),
        name="pack",
    )(place.reshape(-1), cold_row, cold_grads)
    lines = -(-slots // LANES)
    rows = jnp.pad(rows.reshape(devices, slots), ((0, 0), (0, lines * LANES - slots)))
    height = -(-(lines + 1) // 8) * 8
    meta = jnp.concatenate(
        [rows.reshape(devices, lines, LANES),
         jnp.broadcast_to(count[0, :devices, None, None], (devices, height - lines, LANES))], axis=1,
    )
    share = -(-hot // devices)
    partial = jnp.pad(partial, ((0, share * devices - hot), (0, 0))).reshape(devices, share, width)
    me = lax.axis_index("grp") * n_dev + lax.axis_index("dev")
    dma = pltpu.SemaphoreType.DMA
    return pl.pallas_call(
        functools.partial(exchange_kernel, n_grp, n_dev, slots),
        out_shape=jax.ShapeDtypeStruct(table.shape, f32),
        in_specs=[hbm, vmem, vmem, vmem, hbm],
        out_specs=hbm,
        scratch_shapes=[
            pltpu.VMEM((devices, slots, width), f32),
            pltpu.VMEM(meta.shape, i32),
            pltpu.VMEM(partial.shape, f32),
            pltpu.VMEM(partial.shape, f32),
            pltpu.VMEM(table.shape, f32),
            pltpu.VMEM((max(slots, hot), 2 * width), jnp.bfloat16),
            dma, dma((devices,)), dma, dma, dma, dma, dma, dma, dma((2,)),
        ],
        compiler_params=pltpu.CompilerParams(
            collective_id=0, has_side_effects=True, vmem_limit_bytes=48 * 1024 * 1024
        ),
        name="exchange",
    )(send.reshape(devices, slots, width), meta, partial,
      (hot_ids - me * rows_dev).reshape(1, -1), table)


def solution(mesh):
    in_specs = (
        P(("grp", "dev"), None),
        P(("grp", "dev"), None),
        P(("grp", "dev"), None),
        P(("grp", "dev")),
        P(("grp", "dev"), None),
        P(("grp", "dev")),
        P(),
    )
    out_specs = P(("grp", "dev"), None)
    return jax.shard_map(
        functools.partial(on_device, mesh.shape["grp"], mesh.shape["dev"]),
        mesh=mesh, in_specs=in_specs, out_specs=out_specs, check_vma=False,
    )
```

```python
import functools

import jax
import jax.numpy as jnp
from jax import lax
from jax.experimental import pallas as pl
from jax.experimental.pallas import tpu as pltpu
from jax.sharding import PartitionSpec as P

LEARN = 0.05
MESH = pl.DeviceIdType.MESH
LANES = 128
CHUNK = 256
MIB = 1024 * 1024
TILE = 4096


def parts_of(values):
    high = values.astype(jnp.bfloat16)
    rest = values - high.astype(jnp.float32)
    middle = rest.astype(jnp.bfloat16)
    low = (rest - middle.astype(jnp.float32)).astype(jnp.bfloat16)
    return high, middle, low


def plan_kernel(slots, owner_ref, hot_grads_ref, hot_slot_ref, place_ref, count_ref, partial_ref):
    blocks = owner_ref.shape[0] * LANES // CHUNK
    lines = CHUNK // LANES
    tall = count_ref.shape[0]
    before = lax.broadcasted_iota(jnp.int32, (CHUNK, CHUNK), 0)
    after = lax.broadcasted_iota(jnp.int32, (CHUNK, CHUNK), 1)
    tri = (before <= after).astype(jnp.bfloat16)
    owners = lax.broadcasted_iota(jnp.int32, (tall, CHUNK), 0)
    base = owners.astype(jnp.float32)[:, 0:1] * slots - 1.0
    start = base
    for b in range(blocks):
        own = jnp.concatenate([owner_ref[b * lines + j:b * lines + j + 1, :] for j in range(lines)], axis=1)
        hit = own == owners
        run = jnp.dot(hit.astype(jnp.bfloat16), tri, preferred_element_type=jnp.float32) + base
        base = run[:, CHUNK - 1:CHUNK]
        spot = jnp.sum(jnp.where(hit, run, 0.0), axis=0, keepdims=True)
        whole = (spot + 0.5).astype(jnp.int32)
        for j in range(lines):
            r = b * lines + j
            place_ref[r:r + 1, :] = whole[:, j * LANES:(j + 1) * LANES]
    count_ref[...] = jnp.broadcast_to((base - start + 0.5).astype(jnp.int32), count_ref.shape)
    hot, width = partial_ref.shape
    looks = hot_grads_ref.shape[0]
    pick = lax.broadcasted_iota(jnp.int32, (hot, looks), 0) == hot_slot_ref[...]
    split = jnp.concatenate(parts_of(hot_grads_ref[...]), axis=1)
    three = jnp.dot(pick.astype(jnp.bfloat16), split, preferred_element_type=jnp.float32)
    partial_ref[...] = three[:, :width] + three[:, width:2 * width] + three[:, 2 * width:]


def pack_kernel(place_ref, row_ref, grads_ref, send_ref, rows_ref):
    step = 16

    def body(t, carry):
        first = pl.multiple_of(t * step, step)
        for j in range(step):
            to = place_ref[first + j]
            rows_ref[to] = row_ref[first + j]
            send_ref[pl.ds(to, 1), :] = grads_ref[pl.ds(first + j, 1), :]
        return carry

    lax.fori_loop(0, grads_ref.shape[0] // step, body, 0)


def exchange_kernel(
    n_grp, n_dev, slots, send_ref, meta_ref, part_ref, ids_ref, table_ref, out_ref,
    got, gmeta, total, rbuf, acc, halves, s_big, r_big, s_meta, r_meta, s_rs, r_rs, s_ag, r_ag, s_own,
):
    devices = n_grp * n_dev
    width = acc.shape[1]
    rows_dev = acc.shape[0]
    tile = min(TILE, rows_dev)
    me = lax.axis_index("grp") * n_dev + lax.axis_index("dev")
    barrier = pltpu.get_barrier_semaphore()

    def each(fn, first=1, last=devices):
        def body(k, carry):
            p = lax.rem(me + k, devices)
            fn(k, p, (p // n_dev, lax.rem(p, n_dev)))
            return carry
        lax.fori_loop(first, last, body, 0)

    def remote(src, dst, ssem, rsem, where):
        return pltpu.make_async_remote_copy(
            src_ref=src, dst_ref=dst, send_sem=ssem, recv_sem=rsem,
            device_id=where, device_id_type=MESH,
        )

    load = pltpu.make_async_copy(table_ref, acc, s_own.at[0])
    load.start()
    own_big = pltpu.make_async_copy(send_ref.at[me], got.at[me], s_own.at[1])
    own_big.start()
    each(lambda k, p, w: pl.semaphore_signal(barrier, inc=1, device_id=w, device_id_type=MESH))
    pl.semaphore_wait(barrier, devices - 1)

    def big(k, p, w):
        remote(send_ref.at[p], got.at[me], s_big, r_big.at[k], w).start()

    half = devices // 2
    each(lambda k, p, w: remote(part_ref.at[p], rbuf.at[me], s_rs, r_rs, w).start())
    each(lambda k, p, w: remote(meta_ref.at[p], gmeta.at[me], s_meta, r_meta, w).start())
    each(big, 1, half)
    rbuf[me] = part_ref[me]
    gmeta[me] = meta_ref[me]

    here = (lax.axis_index("grp"), lax.axis_index("dev"))
    most = pl.ds(0, devices - 1)

    def all_of(src, dst, ssem, rsem):
        return remote(src.at[most], dst.at[most], ssem, rsem, here)

    rs = all_of(part_ref, rbuf, s_rs, r_rs)
    rs.wait_recv()
    total[me] = jnp.sum(rbuf[...], axis=0)
    each(big, half, half + half // 2)
    rs.wait_send()
    each(lambda k, p, w: remote(total.at[me], total.at[me], s_ag, r_ag, w).start())
    each(big, half + half // 2, devices)

    def add(values, ids):
        count = values.shape[0]
        high = values.astype(jnp.bfloat16)
        halves[0:count, 0:width] = high
        halves[0:count, width:2 * width] = (values - high.astype(jnp.float32)).astype(jnp.bfloat16)
        spot = lax.broadcasted_iota(jnp.int32, (tile, count), 0)

        def body(t, carry):
            at = pl.multiple_of(t * tile, tile)
            hit = jnp.where(spot == ids - at, 1.0, 0.0).astype(jnp.bfloat16)
            both = jnp.dot(hit, halves[0:count, :], preferred_element_type=jnp.float32)
            w = pl.ds(at, tile)
            acc[w, :] = acc[w, :] - LEARN * (both[:, :width] + both[:, width:])
            return carry

        lax.fori_loop(0, rows_dev // tile, body, 0)

    lines = -(-slots // LANES)

    def add_block(source):
        info = gmeta[source]
        filled = info[lines:lines + 1, :]
        ids = jnp.concatenate([info[j:j + 1, :] for j in range(lines)], axis=1)[:, :slots]
        held = jnp.concatenate([filled] * lines, axis=1)[:, :slots]
        ids = jnp.where(lax.broadcasted_iota(jnp.int32, (1, slots), 1) < held, ids, -1)
        block = got[source]
        deep = lax.broadcasted_iota(jnp.int32, block.shape, 0)
        add(jnp.where(deep < filled[:, :width], block, 0.0), ids)

    load.wait()
    own_big.wait()
    add_block(me)
    metas = all_of(meta_ref, gmeta, s_meta, r_meta)
    metas.wait_send()
    metas.wait_recv()

    def arrived(k, carry):
        source = lax.rem(me - k + devices, devices)
        remote(send_ref.at[0], got.at[source], s_big, r_big.at[k], here).wait_recv()
        add_block(source)
        return carry

    lax.fori_loop(1, devices, arrived, 0)
    ag = all_of(total, total, s_ag, r_ag)
    ag.wait_send()
    ag.wait_recv()
    hot = ids_ref.shape[1]
    add(total[...].reshape(-1, width)[:hot], ids_ref[...] - me * rows_dev)
    out = pltpu.make_async_copy(acc, out_ref, s_own.at[0])
    out.start()
    remote(send_ref.at[most], got.at[most], s_big, r_big.at[0], here).wait_send()
    out.wait()


def on_device(n_grp, n_dev, table, cold_grads, cold_owner, cold_row, hot_grads, hot_slot, hot_ids):
    devices = n_grp * n_dev
    width = table.shape[1]
    lookups = cold_grads.shape[0]
    rows_dev = table.shape[0]
    hot = hot_ids.shape[0]
    slots = max(4, 2 * lookups // devices)
    tall = -(-devices // 8) * 8
    vmem, smem, hbm = (pl.BlockSpec(memory_space=m) for m in (pltpu.VMEM, pltpu.SMEM, pl.ANY))
    f32, i32 = jnp.float32, jnp.int32
    place, count, partial = pl.pallas_call(
        functools.partial(plan_kernel, slots),
        out_shape=(
            jax.ShapeDtypeStruct((lookups // LANES, LANES), i32),
            jax.ShapeDtypeStruct((tall, LANES), i32),
            jax.ShapeDtypeStruct((hot, width), f32),
        ),
        in_specs=[vmem] * 3,
        out_specs=(vmem,) * 3,
        compiler_params=pltpu.CompilerParams(vmem_limit_bytes=8 * MIB),
        name="plan",
    )(cold_owner.reshape(-1, LANES), hot_grads, hot_slot.reshape(1, -1))
    send, rows = pl.pallas_call(
        pack_kernel,
        out_shape=(
            jax.ShapeDtypeStruct((devices * slots, width), f32),
            jax.ShapeDtypeStruct((devices * slots,), i32),
        ),
        in_specs=[smem, smem, vmem],
        out_specs=(vmem, smem),
        compiler_params=pltpu.CompilerParams(vmem_limit_bytes=12 * MIB),
        name="pack",
    )(place.reshape(-1), cold_row, cold_grads)
    lines = -(-slots // LANES)
    rows = jnp.pad(rows.reshape(devices, slots), ((0, 0), (0, lines * LANES - slots)))
    height = -(-(lines + 1) // 8) * 8
    meta = jnp.concatenate(
        [rows.reshape(devices, lines, LANES),
         jnp.broadcast_to(count[:devices, None, :], (devices, height - lines, LANES))], axis=1,
    )
    share = -(-hot // devices)
    partial = jnp.pad(partial, ((0, share * devices - hot), (0, 0))).reshape(devices, share, width)
    dma = pltpu.SemaphoreType.DMA
    return pl.pallas_call(
        functools.partial(exchange_kernel, n_grp, n_dev, slots),
        out_shape=jax.ShapeDtypeStruct(table.shape, f32),
        in_specs=[hbm, vmem, vmem, vmem, hbm],
        out_specs=hbm,
        scratch_shapes=[
            pltpu.VMEM((devices, slots, width), f32),
            pltpu.VMEM(meta.shape, i32),
            pltpu.VMEM(partial.shape, f32),
            pltpu.VMEM(partial.shape, f32),
            pltpu.VMEM(table.shape, f32),
            pltpu.VMEM((max(slots, hot), 2 * width), jnp.bfloat16),
            dma, dma((devices,)), dma, dma, dma, dma, dma, dma, dma((2,)),
        ],
        compiler_params=pltpu.CompilerParams(
            collective_id=0, has_side_effects=True, vmem_limit_bytes=32 * MIB
        ),
        name="exchange",
    )(send.reshape(devices, slots, width), meta, partial,
      hot_ids.reshape(1, -1), table)


def solution(mesh):
    in_specs = (
        P(("grp", "dev"), None),
        P(("grp", "dev"), None),
        P(("grp", "dev"), None),
        P(("grp", "dev")),
        P(("grp", "dev"), None),
        P(("grp", "dev")),
        P(),
    )
    out_specs = P(("grp", "dev"), None)
    return jax.shard_map(
        functools.partial(on_device, mesh.shape["grp"], mesh.shape["dev"]),
        mesh=mesh, in_specs=in_specs, out_specs=out_specs, check_vma=False,
    )
```

```python
import functools

import jax
import jax.numpy as jnp
from jax import lax
from jax.experimental import pallas as pl
from jax.experimental.pallas import tpu as pltpu
from jax.sharding import PartitionSpec as P

LEARN = 0.05
MESH = pl.DeviceIdType.MESH
LANES = 128
CHUNK = 256
STEP = 16
MIB = 1024 * 1024
TILE = 4096


def parts_of(values):
    high = values.astype(jnp.bfloat16)
    rest = values - high.astype(jnp.float32)
    middle = rest.astype(jnp.bfloat16)
    low = (rest - middle.astype(jnp.float32)).astype(jnp.bfloat16)
    return high, middle, low


def pack_kernel(
    slots, owner_hbm, row_hbm, grads_hbm, hot_grads_hbm, hot_slot_hbm,
    send_ref, rows_ref, count_ref, partial_ref,
    owner_ref, row_ref, grads_ref, hot_grads_ref, hot_slot_ref, place_ref, place_smem, sem,
):
    copies = [
        pltpu.make_async_copy(a, b, sem.at[i])
        for i, (a, b) in enumerate([
            (owner_hbm, owner_ref), (row_hbm, row_ref), (grads_hbm, grads_ref),
            (hot_grads_hbm, hot_grads_ref), (hot_slot_hbm, hot_slot_ref),
        ])
    ]
    for c in copies:
        c.start()
    copies[0].wait()
    blocks = owner_ref.shape[0] * LANES // CHUNK
    lines = CHUNK // LANES
    tall = count_ref.shape[0]
    before = lax.broadcasted_iota(jnp.int32, (CHUNK, CHUNK), 0)
    after = lax.broadcasted_iota(jnp.int32, (CHUNK, CHUNK), 1)
    tri = (before <= after).astype(jnp.bfloat16)
    owners = lax.broadcasted_iota(jnp.int32, (tall, CHUNK), 0)
    base = owners.astype(jnp.float32)[:, 0:1] * slots - 1.0
    start = base
    for b in range(blocks):
        own = jnp.concatenate([owner_ref[b * lines + j:b * lines + j + 1, :] for j in range(lines)], axis=1)
        hit = own == owners
        run = jnp.dot(hit.astype(jnp.bfloat16), tri, preferred_element_type=jnp.float32) + base
        base = run[:, CHUNK - 1:CHUNK]
        spot = jnp.sum(jnp.where(hit, run, 0.0), axis=0, keepdims=True)
        whole = (spot + 0.5).astype(jnp.int32)
        for j in range(lines):
            r = b * lines + j
            place_ref[r:r + 1, :] = whole[:, j * LANES:(j + 1) * LANES]
    placed = pltpu.make_async_copy(place_ref, place_smem, sem.at[5])
    placed.start()
    count_ref[...] = jnp.broadcast_to((base - start + 0.5).astype(jnp.int32), count_ref.shape)
    copies[3].wait()
    copies[4].wait()
    hot, width = partial_ref.shape
    looks = hot_grads_ref.shape[0]
    pick = lax.broadcasted_iota(jnp.int32, (hot, looks), 0) == hot_slot_ref[...]
    split = jnp.concatenate(parts_of(hot_grads_ref[...]), axis=1)
    three = jnp.dot(pick.astype(jnp.bfloat16), split, preferred_element_type=jnp.float32)
    partial_ref[...] = three[:, :width] + three[:, width:2 * width] + three[:, 2 * width:]
    copies[1].wait()
    copies[2].wait()
    placed.wait()

    def body(line, carry):
        def part(q, c):
            first = pl.multiple_of(q * STEP, STEP)
            for j in range(STEP):
                to = place_smem[line, first + j]
                at = line * LANES + first + j
                rows_ref[to] = row_ref[at]
                send_ref[pl.ds(to, 1), :] = grads_ref[pl.ds(at, 1), :]
            return c

        return lax.fori_loop(0, LANES // STEP, part, carry)

    lax.fori_loop(0, place_ref.shape[0], body, 0)


def partner(at, step, size):
    if size & (size - 1):
        return lax.rem(at + step, size), lax.rem(at - step + size, size)
    mixed = 0
    bit = 1
    while bit < size:
        mixed = mixed + bit * lax.rem(at // bit + step // bit, 2)
        bit *= 2
    return mixed, mixed


def exchange_kernel(
    n_grp, n_dev, slots, send_ref, meta_ref, part_ref, ids_ref, table_ref, acc,
    got, gmeta, total, rbuf, halves, s_big, r_big, s_meta, r_meta, s_rs, r_rs, s_ag, r_ag, s_own,
):
    devices = n_grp * n_dev
    width = acc.shape[1]
    rows_dev = acc.shape[0]
    tile = min(TILE, rows_dev)
    my_grp, my_dev = lax.axis_index("grp"), lax.axis_index("dev")
    me = my_grp * n_dev + my_dev
    barrier = pltpu.get_barrier_semaphore()

    def each(fn, first=1, last=devices):
        def body(k, carry):
            g, d = partner(my_grp, lax.rem(k, n_grp), n_grp)[0], partner(my_dev, k // n_grp, n_dev)[0]
            fn(k, g * n_dev + d, (g, d))
            return carry
        lax.fori_loop(first, last, body, 0)

    def remote(src, dst, ssem, rsem, where):
        return pltpu.make_async_remote_copy(
            src_ref=src, dst_ref=dst, send_sem=ssem, recv_sem=rsem,
            device_id=where, device_id_type=MESH,
        )

    load = pltpu.make_async_copy(table_ref, acc, s_own.at[0])
    load.start()
    own_big = pltpu.make_async_copy(send_ref.at[me], got.at[me], s_own.at[1])
    own_big.start()
    each(lambda k, p, w: pl.semaphore_signal(barrier, inc=1, device_id=w, device_id_type=MESH))
    pl.semaphore_wait(barrier, devices - 1)

    def big(k, p, w):
        remote(send_ref.at[p], got.at[me], s_big, r_big.at[k], w).start()

    most_sent = devices - devices // 4
    each(lambda k, p, w: remote(part_ref.at[p], rbuf.at[me], s_rs, r_rs, w).start())
    each(lambda k, p, w: remote(meta_ref.at[p], gmeta.at[me], s_meta, r_meta, w).start())
    each(big, 1, most_sent)
    rbuf[me] = part_ref[me]
    gmeta[me] = meta_ref[me]

    here = (my_grp, my_dev)
    most = pl.ds(0, devices - 1)

    def all_of(src, dst, ssem, rsem):
        return remote(src.at[most], dst.at[most], ssem, rsem, here)

    rs = all_of(part_ref, rbuf, s_rs, r_rs)
    rs.wait_recv()
    total[me] = jnp.sum(rbuf[...], axis=0)
    rs.wait_send()
    each(lambda k, p, w: remote(total.at[me], total.at[me], s_ag, r_ag, w).start())
    each(big, most_sent, devices)

    def add(values, ids):
        count = values.shape[0]
        high = values.astype(jnp.bfloat16)
        halves[0:count, 0:width] = high
        halves[0:count, width:2 * width] = (values - high.astype(jnp.float32)).astype(jnp.bfloat16)
        spot = lax.broadcasted_iota(jnp.int32, (tile, count), 0)

        def body(t, carry):
            at = pl.multiple_of(t * tile, tile)
            hit = jnp.where(spot == ids - at, 1.0, 0.0).astype(jnp.bfloat16)
            both = jnp.dot(hit, halves[0:count, :], preferred_element_type=jnp.float32)
            w = pl.ds(at, tile)
            acc[w, :] = acc[w, :] - LEARN * (both[:, :width] + both[:, width:])
            return carry

        lax.fori_loop(0, rows_dev // tile, body, 0)

    lines = -(-slots // LANES)

    def add_block(source):
        info = gmeta[source]
        filled = info[lines:lines + 1, :]
        ids = jnp.concatenate([info[j:j + 1, :] for j in range(lines)], axis=1)[:, :slots]
        held = jnp.concatenate([filled] * lines, axis=1)[:, :slots]
        ids = jnp.where(lax.broadcasted_iota(jnp.int32, (1, slots), 1) < held, ids, -1)
        block = got[source]
        deep = lax.broadcasted_iota(jnp.int32, block.shape, 0)
        add(jnp.where(deep < filled[:, :width], block, 0.0), ids)

    load.wait()
    own_big.wait()
    add_block(me)
    metas = all_of(meta_ref, gmeta, s_meta, r_meta)
    metas.wait_send()
    metas.wait_recv()

    def arrived(k, carry):
        g, d = partner(my_grp, lax.rem(k, n_grp), n_grp)[1], partner(my_dev, k // n_grp, n_dev)[1]
        source = g * n_dev + d
        remote(send_ref.at[0], got.at[source], s_big, r_big.at[k], here).wait_recv()
        add_block(source)
        return carry

    lax.fori_loop(1, most_sent, arrived, 0)
    ag = all_of(total, total, s_ag, r_ag)
    ag.wait_send()
    ag.wait_recv()
    hot = ids_ref.shape[1]
    add(total[...].reshape(-1, width)[:hot], ids_ref[...] - me * rows_dev)
    lax.fori_loop(most_sent, devices, arrived, 0)
    remote(send_ref.at[most], got.at[most], s_big, r_big.at[0], here).wait_send()


def on_device(n_grp, n_dev, table, cold_grads, cold_owner, cold_row, hot_grads, hot_slot, hot_ids):
    devices = n_grp * n_dev
    width = table.shape[1]
    lookups = cold_grads.shape[0]
    rows_dev = table.shape[0]
    hot = hot_ids.shape[0]
    slots = max(4, 2 * lookups // devices)
    tall = -(-devices // 8) * 8
    vmem, smem, anywhere, hbm = (
        pl.BlockSpec(memory_space=m) for m in (pltpu.VMEM, pltpu.SMEM, pl.ANY, pltpu.HBM)
    )
    f32, i32 = jnp.float32, jnp.int32
    dma = pltpu.SemaphoreType.DMA
    send, rows, count, partial = pl.pallas_call(
        functools.partial(pack_kernel, slots),
        out_shape=(
            jax.ShapeDtypeStruct((devices * slots, width), f32),
            jax.ShapeDtypeStruct((devices * slots,), i32),
            jax.ShapeDtypeStruct((tall, LANES), i32),
            jax.ShapeDtypeStruct((hot, width), f32),
        ),
        in_specs=[hbm] * 5,
        out_specs=(vmem, smem, vmem, vmem),
        scratch_shapes=[
            pltpu.VMEM((lookups // LANES, LANES), i32),
            pltpu.SMEM((lookups,), i32),
            pltpu.VMEM(cold_grads.shape, f32),
            pltpu.VMEM(hot_grads.shape, f32),
            pltpu.VMEM((1, hot_slot.shape[0]), i32),
            pltpu.VMEM((lookups // LANES, LANES), i32),
            pltpu.SMEM((lookups // LANES, LANES), i32),
            dma((6,)),
        ],
        compiler_params=pltpu.CompilerParams(vmem_limit_bytes=54 * MIB),
        name="pack",
    )(cold_owner.reshape(-1, LANES), cold_row, cold_grads, hot_grads, hot_slot.reshape(1, -1))
    lines = -(-slots // LANES)
    rows = jnp.pad(rows.reshape(devices, slots), ((0, 0), (0, lines * LANES - slots)))
    height = 4 if lines < 4 else -(-(lines + 1) // 8) * 8
    meta = jnp.concatenate(
        [rows.reshape(devices, lines, LANES),
         jnp.broadcast_to(count[:devices, None, :], (devices, height - lines, LANES))], axis=1,
    )
    share = -(-hot // devices)
    partial = jnp.pad(partial, ((0, share * devices - hot), (0, 0))).reshape(devices, share, width)
    return pl.pallas_call(
        functools.partial(exchange_kernel, n_grp, n_dev, slots),
        out_shape=jax.ShapeDtypeStruct(table.shape, f32),
        in_specs=[anywhere, vmem, vmem, vmem, hbm],
        out_specs=vmem,
        scratch_shapes=[
            pltpu.VMEM((devices, slots, width), f32),
            pltpu.VMEM(meta.shape, i32),
            pltpu.VMEM(partial.shape, f32),
            pltpu.VMEM(partial.shape, f32),
            pltpu.VMEM((max(slots, hot), 2 * width), jnp.bfloat16),
            dma, dma((devices,)), dma, dma, dma, dma, dma, dma, dma((2,)),
        ],
        compiler_params=pltpu.CompilerParams(
            collective_id=0, has_side_effects=True, vmem_limit_bytes=48 * MIB
        ),
        name="exchange",
    )(send.reshape(devices, slots, width), meta, partial,
      hot_ids.reshape(1, -1), table)


def solution(mesh):
    in_specs = (
        P(("grp", "dev"), None),
        P(("grp", "dev"), None),
        P(("grp", "dev"), None),
        P(("grp", "dev")),
        P(("grp", "dev"), None),
        P(("grp", "dev")),
        P(),
    )
    out_specs = P(("grp", "dev"), None)
    return jax.shard_map(
        functools.partial(on_device, mesh.shape["grp"], mesh.shape["dev"]),
        mesh=mesh, in_specs=in_specs, out_specs=out_specs, check_vma=False,
    )
```

```python
import functools

import jax
import jax.numpy as jnp
from jax import lax
from jax.experimental import pallas as pl
from jax.experimental.pallas import tpu as pltpu
from jax.sharding import PartitionSpec as P

LEARN = 0.05
MESH = pl.DeviceIdType.MESH
LANES = 128
CHUNK = 256
MIB = 1024 * 1024
TILE = 4096


def parts_of(values):
    high = values.astype(jnp.bfloat16)
    rest = values - high.astype(jnp.float32)
    middle = rest.astype(jnp.bfloat16)
    low = (rest - middle.astype(jnp.float32)).astype(jnp.bfloat16)
    return high, middle, low


def plan_kernel(slots, owner_ref, hot_grads_ref, hot_slot_ref, place_ref, count_ref, partial_ref):
    blocks = owner_ref.shape[0] * LANES // CHUNK
    lines = CHUNK // LANES
    tall = count_ref.shape[0]
    before = lax.broadcasted_iota(jnp.int32, (CHUNK, CHUNK), 0)
    after = lax.broadcasted_iota(jnp.int32, (CHUNK, CHUNK), 1)
    tri = (before <= after).astype(jnp.bfloat16)
    owners = lax.broadcasted_iota(jnp.int32, (tall, CHUNK), 0)
    base = owners.astype(jnp.float32)[:, 0:1] * slots - 1.0
    start = base
    for b in range(blocks):
        own = jnp.concatenate([owner_ref[b * lines + j:b * lines + j + 1, :] for j in range(lines)], axis=1)
        hit = own == owners
        run = jnp.dot(hit.astype(jnp.bfloat16), tri, preferred_element_type=jnp.float32) + base
        base = run[:, CHUNK - 1:CHUNK]
        spot = jnp.sum(jnp.where(hit, run, 0.0), axis=0, keepdims=True)
        whole = (spot + 0.5).astype(jnp.int32)
        for j in range(lines):
            r = b * lines + j
            place_ref[r:r + 1, :] = whole[:, j * LANES:(j + 1) * LANES]
    count_ref[...] = jnp.broadcast_to((base - start + 0.5).astype(jnp.int32), count_ref.shape)
    hot, width = partial_ref.shape
    looks = hot_grads_ref.shape[0]
    pick = lax.broadcasted_iota(jnp.int32, (hot, looks), 0) == hot_slot_ref[...]
    split = jnp.concatenate(parts_of(hot_grads_ref[...]), axis=1)
    three = jnp.dot(pick.astype(jnp.bfloat16), split, preferred_element_type=jnp.float32)
    partial_ref[...] = three[:, :width] + three[:, width:2 * width] + three[:, 2 * width:]


def pack_kernel(place_ref, row_ref, grads_ref, send_ref, rows_ref):
    step = 16

    def body(t, carry):
        first = pl.multiple_of(t * step, step)
        for j in range(step):
            to = place_ref[first + j]
            rows_ref[to] = row_ref[first + j]
            send_ref[pl.ds(to, 1), :] = grads_ref[pl.ds(first + j, 1), :]
        return carry

    lax.fori_loop(0, grads_ref.shape[0] // step, body, 0)


def partner(at, step, size):
    if size & (size - 1):
        return lax.rem(at + step, size), lax.rem(at - step + size, size)
    mixed = 0
    bit = 1
    while bit < size:
        mixed = mixed + bit * lax.rem(at // bit + step // bit, 2)
        bit *= 2
    return mixed, mixed


def exchange_kernel(
    n_grp, n_dev, slots, send_ref, meta_ref, part_ref, ids_ref, table_ref, acc,
    got, gmeta, total, rbuf, halves, s_big, r_big, s_meta, r_meta, s_rs, r_rs, s_ag, r_ag, s_own,
):
    devices = n_grp * n_dev
    width = acc.shape[1]
    rows_dev = acc.shape[0]
    tile = min(TILE, rows_dev)
    my_grp, my_dev = lax.axis_index("grp"), lax.axis_index("dev")
    me = my_grp * n_dev + my_dev
    barrier = pltpu.get_barrier_semaphore()

    def each(fn, first=1, last=devices):
        def body(k, carry):
            g, d = partner(my_grp, lax.rem(k, n_grp), n_grp)[0], partner(my_dev, k // n_grp, n_dev)[0]
            fn(k, g * n_dev + d, (g, d))
            return carry
        lax.fori_loop(first, last, body, 0)

    def remote(src, dst, ssem, rsem, where):
        return pltpu.make_async_remote_copy(
            src_ref=src, dst_ref=dst, send_sem=ssem, recv_sem=rsem,
            device_id=where, device_id_type=MESH,
        )

    load = pltpu.make_async_copy(table_ref, acc, s_own.at[0])
    load.start()
    own_big = pltpu.make_async_copy(send_ref.at[me], got.at[me], s_own.at[1])
    own_big.start()
    each(lambda k, p, w: pl.semaphore_signal(barrier, inc=1, device_id=w, device_id_type=MESH))
    pl.semaphore_wait(barrier, devices - 1)

    def big(k, p, w):
        remote(send_ref.at[p], got.at[me], s_big, r_big.at[k], w).start()

    most_sent = devices - devices // 4
    each(lambda k, p, w: remote(part_ref.at[p], rbuf.at[me], s_rs, r_rs, w).start())
    each(lambda k, p, w: remote(meta_ref.at[p], gmeta.at[me], s_meta, r_meta, w).start())
    each(big, 1, most_sent)
    rbuf[me] = part_ref[me]
    gmeta[me] = meta_ref[me]

    here = (my_grp, my_dev)
    most = pl.ds(0, devices - 1)

    def all_of(src, dst, ssem, rsem):
        return remote(src.at[most], dst.at[most], ssem, rsem, here)

    rs = all_of(part_ref, rbuf, s_rs, r_rs)
    rs.wait_recv()
    total[me] = jnp.sum(rbuf[...], axis=0)
    rs.wait_send()
    each(lambda k, p, w: remote(total.at[me], total.at[me], s_ag, r_ag, w).start())
    each(big, most_sent, devices)

    def add(values, ids):
        count = values.shape[0]
        high = values.astype(jnp.bfloat16)
        halves[0:count, 0:width] = high
        halves[0:count, width:2 * width] = (values - high.astype(jnp.float32)).astype(jnp.bfloat16)
        spot = lax.broadcasted_iota(jnp.int32, (tile, count), 0)

        def body(t, carry):
            at = pl.multiple_of(t * tile, tile)
            hit = jnp.where(spot == ids - at, 1.0, 0.0).astype(jnp.bfloat16)
            both = jnp.dot(hit, halves[0:count, :], preferred_element_type=jnp.float32)
            w = pl.ds(at, tile)
            acc[w, :] = acc[w, :] - LEARN * (both[:, :width] + both[:, width:])
            return carry

        lax.fori_loop(0, rows_dev // tile, body, 0)

    lines = -(-slots // LANES)

    def add_block(source):
        info = gmeta[source]
        filled = info[lines:lines + 1, :]
        ids = jnp.concatenate([info[j:j + 1, :] for j in range(lines)], axis=1)[:, :slots]
        held = jnp.concatenate([filled] * lines, axis=1)[:, :slots]
        ids = jnp.where(lax.broadcasted_iota(jnp.int32, (1, slots), 1) < held, ids, -1)
        block = got[source]
        deep = lax.broadcasted_iota(jnp.int32, block.shape, 0)
        add(jnp.where(deep < filled[:, :width], block, 0.0), ids)

    load.wait()
    own_big.wait()
    add_block(me)
    metas = all_of(meta_ref, gmeta, s_meta, r_meta)
    metas.wait_send()
    metas.wait_recv()

    def arrived(k, carry):
        g, d = partner(my_grp, lax.rem(k, n_grp), n_grp)[1], partner(my_dev, k // n_grp, n_dev)[1]
        source = g * n_dev + d
        remote(send_ref.at[0], got.at[source], s_big, r_big.at[k], here).wait_recv()
        add_block(source)
        return carry

    lax.fori_loop(1, most_sent, arrived, 0)
    ag = all_of(total, total, s_ag, r_ag)
    ag.wait_send()
    ag.wait_recv()
    hot = ids_ref.shape[1]
    add(total[...].reshape(-1, width)[:hot], ids_ref[...] - me * rows_dev)
    lax.fori_loop(most_sent, devices, arrived, 0)
    remote(send_ref.at[most], got.at[most], s_big, r_big.at[0], here).wait_send()


def on_device(n_grp, n_dev, table, cold_grads, cold_owner, cold_row, hot_grads, hot_slot, hot_ids):
    devices = n_grp * n_dev
    width = table.shape[1]
    lookups = cold_grads.shape[0]
    rows_dev = table.shape[0]
    hot = hot_ids.shape[0]
    slots = max(4, 2 * lookups // devices)
    tall = -(-devices // 8) * 8
    vmem, smem, hbm = (pl.BlockSpec(memory_space=m) for m in (pltpu.VMEM, pltpu.SMEM, pl.ANY))
    f32, i32 = jnp.float32, jnp.int32
    place, count, partial = pl.pallas_call(
        functools.partial(plan_kernel, slots),
        out_shape=(
            jax.ShapeDtypeStruct((lookups // LANES, LANES), i32),
            jax.ShapeDtypeStruct((tall, LANES), i32),
            jax.ShapeDtypeStruct((hot, width), f32),
        ),
        in_specs=[vmem] * 3,
        out_specs=(vmem,) * 3,
        compiler_params=pltpu.CompilerParams(vmem_limit_bytes=8 * MIB),
        cost_estimate=pl.CostEstimate(flops=0, bytes_accessed=4 * MIB, transcendentals=0),
        name="plan",
    )(cold_owner.reshape(-1, LANES), hot_grads, hot_slot.reshape(1, -1))
    send, rows = pl.pallas_call(
        pack_kernel,
        out_shape=(
            jax.ShapeDtypeStruct((devices * slots, width), f32),
            jax.ShapeDtypeStruct((devices * slots,), i32),
        ),
        in_specs=[smem, smem, vmem],
        out_specs=(vmem, smem),
        compiler_params=pltpu.CompilerParams(vmem_limit_bytes=12 * MIB),
        cost_estimate=pl.CostEstimate(flops=0, bytes_accessed=24 * MIB, transcendentals=0),
        name="pack",
    )(place.reshape(-1), cold_row, cold_grads)
    lines = -(-slots // LANES)
    rows = jnp.pad(rows.reshape(devices, slots), ((0, 0), (0, lines * LANES - slots)))
    height = 4 if lines < 4 else -(-(lines + 1) // 8) * 8
    meta = jnp.concatenate(
        [rows.reshape(devices, lines, LANES),
         jnp.broadcast_to(count[:devices, None, :], (devices, height - lines, LANES))], axis=1,
    )
    share = -(-hot // devices)
    partial = jnp.pad(partial, ((0, share * devices - hot), (0, 0))).reshape(devices, share, width)
    dma = pltpu.SemaphoreType.DMA
    return pl.pallas_call(
        functools.partial(exchange_kernel, n_grp, n_dev, slots),
        out_shape=jax.ShapeDtypeStruct(table.shape, f32),
        in_specs=[hbm, vmem, vmem, vmem, hbm],
        out_specs=vmem,
        scratch_shapes=[
            pltpu.VMEM((devices, slots, width), f32),
            pltpu.VMEM(meta.shape, i32),
            pltpu.VMEM(partial.shape, f32),
            pltpu.VMEM(partial.shape, f32),
            pltpu.VMEM((max(slots, hot), 2 * width), jnp.bfloat16),
            dma, dma((devices,)), dma, dma, dma, dma, dma, dma, dma((2,)),
        ],
        compiler_params=pltpu.CompilerParams(
            collective_id=0, has_side_effects=True, vmem_limit_bytes=32 * MIB
        ),
        name="exchange",
    )(send.reshape(devices, slots, width), meta, partial,
      hot_ids.reshape(1, -1), table)


def solution(mesh):
    in_specs = (
        P(("grp", "dev"), None),
        P(("grp", "dev"), None),
        P(("grp", "dev"), None),
        P(("grp", "dev")),
        P(("grp", "dev"), None),
        P(("grp", "dev")),
        P(),
    )
    out_specs = P(("grp", "dev"), None)
    return jax.shard_map(
        functools.partial(on_device, mesh.shape["grp"], mesh.shape["dev"]),
        mesh=mesh, in_specs=in_specs, out_specs=out_specs, check_vma=False,
    )
```
